32 devices in a mesh: data: 1 (over z), pp: 4 (over y), ep: 8 (over x, core).
Axes of the slice: x: 4, y: 4, z: 1, core: 2. Of those that a mesh axis runs over, the one named last changes fastest.
The devices are a block of a 4x4x8 slice.
Arguments:
- expert_out: bfloat16 [4, 32, 2880, 1024], P(('data', 'pp'), 'ep')
- expert_ids: int32 [4, 24, 384, 8], P(('data', 'pp'), 'ep')
- slot_ids: int32 [4, 24, 384, 8], P(('data', 'pp'), 'ep')
- gate_vals: float32 [4, 24, 384, 8], P(('data', 'pp'), 'ep')
- residual: bfloat16 [4, 24, 384, 1024], P(('data', 'pp'), 'ep')
- norm_scale: float32 [4, 1024], P('pp')
- w_query: bfloat16 [4, 1024, 16, 64], P('pp')
- w_key: bfloat16 [4, 1024, 16, 64], P('pp')
- w_value: bfloat16 [4, 1024, 16, 64], P('pp')
- w_out: bfloat16 [4, 16, 64, 1024], P('pp')
Outputs:
- output: bfloat16 [4, 24, 384, 1024], P(('data', 'pp'), 'ep')
All inputs are finite; a program needn't handle non-finite values.
Results may differ from the reference program's by a relative error of at most 0.02.
Values are sent between devices in bfloat16 or wider.
A program may use at most 768 MiB of HBM per device.

```python
import jax
import jax.numpy as jnp
from jax import lax

STAGES = 4
EP_DEVS = 8
SEQS_DEV = 3
SEQ_LEN = 384
D = 1024
HEADS = 16
HEAD = 64
EXPERTS = 32
TOP = 8
CAP_DEV = 360

NUM_SEQ = EP_DEVS * SEQS_DEV
TOKENS = NUM_SEQ * SEQ_LEN
TOK_DEV = SEQS_DEV * SEQ_LEN
CAPACITY = EP_DEVS * CAP_DEV
HIDDEN = HEADS * HEAD
NORM_EPS = 1e-6


def queue_pos(flat_ids):
    sort_order = jnp.argsort(flat_ids, stable=True)
    ordered = flat_ids[sort_order]
    first_pos = jnp.searchsorted(ordered, ordered, side='left')
    rank_sorted = jnp.arange(flat_ids.shape[0]) - first_pos
    return rank_sorted[jnp.argsort(sort_order, stable=True)]


def draw_routing(route_key):
    rank_key, noise_key = jax.random.split(route_key)
    rank_draw = jax.random.randint(rank_key, (STAGES, EXPERTS), 0, 1 << 20) * EXPERTS + jnp.arange(EXPERTS)
    expert_rank = jnp.argsort(rank_draw, axis=-1)
    hot_bias = jnp.where(expert_rank == 0, 4000, jnp.where(expert_rank < 3, 200, 0))
    stage_keys = jax.random.split(noise_key, STAGES)

    def pick_stage(stage_args):
        stage_key, stage_bias = stage_args
        score_noise = jax.random.randint(stage_key, (TOKENS, EXPERTS), 0, 1000)
        score_total = (score_noise + stage_bias) * EXPERTS + jnp.arange(EXPERTS)
        return lax.top_k(score_total, TOP)[1]

    expert_ids = lax.map(pick_stage, (stage_keys, hot_bias)).astype(jnp.int32)
    positions = jax.vmap(queue_pos)(expert_ids.reshape(STAGES * EP_DEVS, TOK_DEV * TOP))
    positions = positions.reshape(STAGES, NUM_SEQ, SEQ_LEN, TOP)
    owner_dev = (jnp.arange(NUM_SEQ) // SEQS_DEV)[None, :, None, None]
    slot_ids = jnp.where(positions < CAP_DEV, owner_dev * CAP_DEV + positions, -1).astype(jnp.int32)
    return expert_ids.reshape(STAGES, NUM_SEQ, SEQ_LEN, TOP), slot_ids


def setup_inputs(seed: int = 0, part: int = 0) -> dict:
    base_key = jax.random.key(seed)
    part_key = jax.random.fold_in(base_key, part)
    route_key, out_key, gain_key, mean_key, gate_key, resid_key = jax.random.split(part_key, 6)
    norm_key, q_key, k_key, v_key, o_key = jax.random.split(base_key, 5)
    expert_ids, slot_ids = draw_routing(route_key)
    expert_gain = jnp.exp(0.6 * jax.random.normal(gain_key, (STAGES, EXPERTS, 1, 1), jnp.float32))
    expert_mean = 0.7 * jax.random.normal(mean_key, (STAGES, EXPERTS, 1, D), jnp.float32)
    expert_out = (expert_mean + expert_gain * jax.random.normal(out_key, (STAGES, EXPERTS, CAPACITY, D), jnp.float32)).astype(jnp.bfloat16)
    gate_vals = jax.nn.softmax(2.0 * jax.random.normal(gate_key, (STAGES, NUM_SEQ, SEQ_LEN, TOP), jnp.float32), axis=-1).astype(jnp.float32)
    residual = jax.random.normal(resid_key, (STAGES, NUM_SEQ, SEQ_LEN, D), jnp.float32).astype(jnp.bfloat16)
    norm_scale = jnp.exp(0.5 * jax.random.normal(norm_key, (STAGES, D), jnp.float32)).astype(jnp.float32)
    w_query = (1.3 * D ** -0.5 * jax.random.normal(q_key, (STAGES, D, HEADS, HEAD), jnp.float32)).astype(jnp.bfloat16)
    w_key = (1.3 * D ** -0.5 * jax.random.normal(k_key, (STAGES, D, HEADS, HEAD), jnp.float32)).astype(jnp.bfloat16)
    w_value = (D ** -0.5 * jax.random.normal(v_key, (STAGES, D, HEADS, HEAD), jnp.float32)).astype(jnp.bfloat16)
    w_out = (3.0 * HIDDEN ** -0.5 * jax.random.normal(o_key, (STAGES, HEADS, HEAD, D), jnp.float32)).astype(jnp.bfloat16)
    return {'expert_out': expert_out, 'expert_ids': expert_ids, 'slot_ids': slot_ids, 'gate_vals': gate_vals, 'residual': residual, 'norm_scale': norm_scale, 'w_query': w_query, 'w_key': w_key, 'w_value': w_value, 'w_out': w_out}


def combine_rows(expert_table, ids_seq, slots_seq, gates_seq, resid_seq):
    kept_mask = slots_seq >= 0
    picked_rows = expert_table[ids_seq, jnp.where(kept_mask, slots_seq, 0)].astype(jnp.float32)
    gate_used = jnp.where(kept_mask, gates_seq, 0.0)
    merged = resid_seq.astype(jnp.float32) + jnp.sum(gate_used[..., None] * picked_rows, axis=1)
    return merged.astype(jnp.bfloat16)


def attn_block(merged, scale_vec, q_mat, k_mat, v_mat, o_mat):
    resid_f32 = merged.astype(jnp.float32)
    inv_rms = lax.rsqrt(jnp.mean(resid_f32 * resid_f32, axis=-1, keepdims=True) + NORM_EPS)
    normed_in = (resid_f32 * inv_rms * scale_vec).astype(jnp.bfloat16)

    def project(w_mat):
        product = jnp.dot(normed_in, w_mat, preferred_element_type=jnp.float32).astype(jnp.bfloat16)
        return product.reshape(SEQ_LEN, HEADS, HEAD).astype(jnp.float32)

    q_heads = project(q_mat)
    k_heads = project(k_mat)
    v_heads = project(v_mat)
    scores = jnp.einsum('qhe,khe->hqk', q_heads, k_heads) * HEAD ** -0.5
    causal = jnp.arange(SEQ_LEN)[:, None] >= jnp.arange(SEQ_LEN)[None, :]
    scores = jnp.where(causal, scores, -1e30)
    exp_scores = jnp.exp(scores - jnp.max(scores, axis=-1, keepdims=True))
    row_sums = jnp.sum(exp_scores, axis=-1)
    mixed_vals = jnp.einsum('hqk,khe->qhe', exp_scores.astype(jnp.bfloat16).astype(jnp.float32), v_heads)
    attn_out = (mixed_vals / row_sums.T[:, :, None]).astype(jnp.bfloat16).reshape(SEQ_LEN, HIDDEN)
    proj_out = jnp.dot(attn_out, o_mat, preferred_element_type=jnp.float32).astype(jnp.bfloat16)
    return (resid_f32 + proj_out.astype(jnp.float32)).astype(jnp.bfloat16)


def reference(expert_out, expert_ids, slot_ids, gate_vals, residual, norm_scale, w_query, w_key, w_value, w_out):
    def one_stage(stage_idx):
        prev_stage = (stage_idx + STAGES - 1) % STAGES
        expert_table = expert_out[prev_stage]
        scale_vec = norm_scale[stage_idx]
        q_mat = w_query[stage_idx].reshape(D, HIDDEN)
        k_mat = w_key[stage_idx].reshape(D, HIDDEN)
        v_mat = w_value[stage_idx].reshape(D, HIDDEN)
        o_mat = w_out[stage_idx].reshape(HIDDEN, D)

        def one_seq(seq_idx):
            merged = combine_rows(expert_table, expert_ids[prev_stage, seq_idx], slot_ids[prev_stage, seq_idx], gate_vals[prev_stage, seq_idx], residual[prev_stage, seq_idx])
            return attn_block(merged, scale_vec, q_mat, k_mat, v_mat, o_mat)

        return lax.map(one_seq, jnp.arange(NUM_SEQ))

    return lax.map(one_stage, jnp.arange(STAGES))
```

```python
import functools

import jax
import jax.numpy as jnp
from jax import lax
from jax.experimental import pallas as pl
from jax.experimental.pallas import tpu as pltpu
from jax.sharding import PartitionSpec as P

NORM_EPS = 1e-6
CORES = 2
F32 = jnp.float32
BF16 = jnp.bfloat16
MESH = pl.DeviceIdType.MESH
NT = (((1,), (1,)), ((), ()))
SUBS = 3


def combine_kernel(dims, table, rows_hbm, resid_hbm, out_hbm, meta, own_rows, sib_rows, part, hop_in, dir_in, last_in,
                   resid, y_buf, meta_s, meta_r, sib_s, sib_r, own_sem, res_sem, hop_s, hop_r, dir_s, dir_r, last_s, last_r,
                   y_s, y_r):
    chips, stages, seqs, seq_len, cap, local = dims
    half = seq_len // 2
    sub = half // SUBS
    ep = lax.axis_index('ep')
    stage = lax.axis_index('pp')
    chip, core = ep // CORES, ep % CORES

    def dev(delta):
        return {'ep': ((chip + delta) % chips) * CORES + core}

    sibling = {'ep': chip * CORES + 1 - core}
    up = {'pp': (stage + 1) % stages}
    down = {'pp': (stage + stages - 1) % stages}
    right, left = dev(1), dev(chips - 1)

    def rows_of(rel, which):
        owner = ((chip + rel) % chips) * CORES + which
        return rows_hbm.at[:, pl.ds(pl.multiple_of(owner * cap, 8), cap), :]

    def meta_copy(rel):
        return pltpu.make_async_remote_copy(src_ref=table.at[(chip + chips - rel) % chips], dst_ref=meta.at[rel], send_sem=meta_s.at[rel],
                                            recv_sem=meta_r.at[rel], device_id=dev(chips - rel), device_id_type=MESH)

    def sib_copy(rel):
        return pltpu.make_async_remote_copy(src_ref=rows_of(rel, 1 - core), dst_ref=sib_rows.at[rel], send_sem=sib_s.at[rel],
                                            recv_sem=sib_r.at[rel], device_id=sibling, device_id_type=MESH)

    def own_copy(rel, slot):
        return pltpu.make_async_copy(rows_of(rel, core), own_rows.at[slot], own_sem.at[slot])

    def ring_copy(src, dst, ssem, rsem, way):
        return pltpu.make_async_remote_copy(src_ref=src, dst_ref=dst, send_sem=ssem, recv_sem=rsem,
                                            device_id=right if way == 0 else left, device_id_type=MESH)

    def hop_copy(way, s):
        return ring_copy(part.at[2, s, way], hop_in.at[way, s], hop_s.at[way, s], hop_r.at[way, s], way)

    def dir_copy(way, s):
        rel = 1 if way == 0 else chips - 1
        return ring_copy(part.at[rel, s, 1 - way], dir_in.at[way, s], dir_s.at[way, s], dir_r.at[way, s], way)

    def last_copy(way, s, u):
        rel = 1 if way == 0 else chips - 1
        span = pl.ds(pl.multiple_of(u * sub, 8), sub)
        return ring_copy(part.at[rel, s, way, span], last_in.at[way, s, span], last_s.at[way, s, u], last_r.at[way, s, u], way)

    def y_copy(s, w, u):
        span = pl.ds(pl.multiple_of(w * half + u * sub, 8), sub)
        return pltpu.make_async_remote_copy(src_ref=y_buf.at[s, span], dst_ref=out_hbm.at[s, span], send_sem=y_s.at[s, w, u],
                                            recv_sem=y_r.at[s, w, u], device_id=up, device_id_type=MESH)

    def order(k):
        return (2 + 3 * k) % chips

    own_copy(2, 0).start()
    res_copy = pltpu.make_async_copy(resid_hbm, resid, res_sem)
    res_copy.start()

    barrier = pltpu.get_barrier_semaphore()
    peers = (sibling, right, left, dev(2), up, down)
    for peer in peers:
        pl.semaphore_signal(barrier, inc=1, device_id=peer, device_id_type=MESH)
    pl.semaphore_wait(barrier, len(peers))

    for rel in (2, 3, 1):
        meta_copy(rel).start()
    for k in range(chips):
        sib_copy(order(k)).start()

    slot_iota = lax.broadcasted_iota(jnp.int32, (seq_len, cap), 1).astype(F32)

    def combine_step(n, carry):
        k, s = n // seqs, n % seqs
        rel = order(k)
        slot = k % 2

        @pl.when(s == 0)
        def _():
            own_copy(rel, slot).wait()
            sib_copy(rel).wait_recv()

            @pl.when(k < chips - 1)
            def _():
                own_copy(order(k + 1), 1 - slot).start()

            @pl.when(rel != 0)
            def _():
                meta_copy(rel).wait_recv()

            @pl.when(rel == 0)
            def _():
                meta[0] = table[chip]

        slots = meta[rel, 0, s].T
        gates = meta[rel, 1, s].T
        for e in range(CORES * local):
            pick = jnp.where(slots[:, e:e + 1] == slot_iota, 1.0, 0.0).astype(BF16)
            rows = own_rows[slot, e] if e < local else sib_rows[rel, e - local]
            term = gates[:, e:e + 1] * jnp.dot(pick, rows, preferred_element_type=F32)
            for w in range(2):
                piece = term[w * half:(w + 1) * half]
                if e == 0:
                    part[rel, s, w] = piece
                else:
                    part[rel, s, w] += piece

        @pl.when(rel == 2)
        def _():
            hop_copy(0, s).start()
            hop_copy(1, s).start()

        @pl.when(rel == 1)
        def _():
            dir_copy(0, s).start()

        @pl.when(rel == chips - 1)
        def _():
            dir_copy(1, s).start()

        return carry

    lax.fori_loop(0, chips * seqs, combine_step, 0)
    res_copy.wait()

    def relay_step(s, carry):
        for way in range(2):
            rel = 1 if way == 0 else chips - 1
            hop_copy(way, s).wait_recv()
            part[rel, s, way] += hop_in[way, s]
            for u in range(SUBS):
                last_copy(way, s, u).start()
        return carry

    lax.fori_loop(0, seqs, relay_step, 0)

    def final_step(n, carry):
        s, u = n // SUBS, n % SUBS
        span = pl.ds(pl.multiple_of(u * sub, 8), sub)

        @pl.when(u == 0)
        def _():
            dir_copy(0, s).wait_recv()
            dir_copy(1, s).wait_recv()

        for w in range(2):
            last_copy(w, s, u).wait_recv()
            whole = pl.ds(pl.multiple_of(w * half + u * sub, 8), sub)
            total = resid[s, whole].astype(F32) + part[0, s, w, span] + dir_in[1 - w, s, span] + last_in[w, s, span]
            y_buf[s, whole] = total.astype(BF16)
            y_copy(s, w, u).start()
        return carry

    lax.fori_loop(0, seqs * SUBS, final_step, 0)

    def drain(s, carry):
        for way in range(2):
            hop_copy(way, s).wait_send()
            dir_copy(way, s).wait_send()
            for u in range(SUBS):
                last_copy(way, s, u).wait_send()
                y_copy(s, way, u).wait()
        return carry

    for rel in (2, 3, 1):
        meta_copy(rel).wait_send()
    for k in range(chips):
        sib_copy(order(k)).wait_send()
    lax.fori_loop(0, seqs, drain, 0)


def attn_kernel(head_dim, y_ref, scale_ref, wq_ref, wk_ref, wv_ref, wo_ref, z_ref, q_buf, k_buf, v_buf, a_buf):
    seq_len, width = y_ref.shape
    pair = 2 * head_dim
    block = 128
    resid = y_ref[...].astype(F32)
    inv_rms = lax.rsqrt(jnp.mean(resid * resid, axis=-1, keepdims=True) + NORM_EPS)
    x = (resid * inv_rms * scale_ref[...]).astype(BF16)
    for w_ref, buf in ((wq_ref, q_buf), (wk_ref, k_buf), (wv_ref, v_buf)):
        buf[...] = lax.dot_general(x, w_ref[...], NT, preferred_element_type=F32).astype(BF16)
    low = lax.broadcasted_iota(jnp.int32, (block, pair), 1) < head_dim
    causal = lax.broadcasted_iota(jnp.int32, (block, block), 0) >= lax.broadcasted_iota(jnp.int32, (block, block), 1)

    def pair_step(p, carry):
        cols = pl.ds(pl.multiple_of(p * pair, pair), pair)
        for qb in range(seq_len // block):
            rows = slice(qb * block, (qb + 1) * block)
            keys = (qb + 1) * block
            q_pair = q_buf[rows, cols]
            k_pair = k_buf[0:keys, cols]
            v_pair = v_buf[0:keys, cols]
            outs = []
            for h in range(2):
                keep = low if h == 0 else jnp.logical_not(low)
                q_one = jnp.where(keep, q_pair.astype(F32), 0.0).astype(BF16)
                scores = lax.dot_general(q_one, k_pair, NT, preferred_element_type=F32) * (head_dim ** -0.5)
                diag = jnp.where(causal, scores[:, keys - block:], -1e30)
                scores = diag if qb == 0 else jnp.concatenate([scores[:, :keys - block], diag], axis=1)
                probs = jnp.exp(scores - jnp.max(scores, axis=-1, keepdims=True))
                sums = jnp.sum(probs, axis=-1, keepdims=True)
                outs.append(jnp.dot(probs.astype(BF16), v_pair, preferred_element_type=F32) / sums)
            a_buf[rows, cols] = jnp.where(low, outs[0], outs[1]).astype(BF16)
        return carry

    lax.fori_loop(0, width // pair, pair_step, 0)
    proj = jnp.dot(a_buf[...], wo_ref[...], preferred_element_type=F32).astype(BF16)
    z_ref[...] = (y_ref[...].astype(F32) + proj.astype(F32)).astype(BF16)


def solution(mesh):
    ep_size, pp_size = mesh.shape['ep'], mesh.shape['pp']
    chips = ep_size // CORES
    token_spec = P(('data', 'pp'), 'ep', None, None)
    weight_spec = P('pp', None, None, None)

    def body(expert_out, expert_ids, slot_ids, gate_vals, residual, norm_scale, w_query, w_key, w_value, w_out):
        local, capacity, width = expert_out.shape[1:]
        cap = capacity // ep_size
        seqs, seq_len = residual.shape[1:3]
        half, sub = seq_len // 2, seq_len // 2 // SUBS
        heads, head_dim = w_query.shape[2:]
        ep = lax.axis_index('ep')
        ids, slots, gates = (jnp.swapaxes(a[0], 1, 2)[None] for a in (expert_ids, slot_ids, gate_vals))
        number = jnp.arange(chips * CORES * local)
        core_flip = (number // local % CORES + ep % CORES) % CORES
        expert = (number // (CORES * local) * CORES + core_flip) * local + number % local
        match = (ids == expert[:, None, None, None]) & (slots >= 0)
        slot_of = jnp.max(jnp.where(match, slots - ep * cap, -1), axis=2).astype(F32)
        gate_of = jnp.sum(jnp.where(match, gates, 0.0), axis=2)
        table = jnp.stack([slot_of, gate_of]).reshape(2, chips, CORES * local, seqs, seq_len).transpose(1, 0, 3, 2, 4)

        dims = (chips, pp_size, seqs, seq_len, cap, local)
        dma = pltpu.SemaphoreType.DMA
        any_spec = pl.BlockSpec(memory_space=pl.ANY)
        vmem_spec = pl.BlockSpec(memory_space=pltpu.VMEM)
        arrived = pl.pallas_call(
            functools.partial(combine_kernel, dims),
            out_shape=jax.ShapeDtypeStruct((seqs, seq_len, width), BF16),
            in_specs=[vmem_spec, any_spec, any_spec],
            out_specs=any_spec,
            scratch_shapes=[
                pltpu.VMEM((chips, 2, seqs, CORES * local, seq_len), F32),
                pltpu.VMEM((2, local, cap, width), BF16),
                pltpu.VMEM((chips, local, cap, width), BF16),
                pltpu.VMEM((chips, seqs, 2, half, width), F32),
                pltpu.VMEM((2, seqs, half, width), F32),
                pltpu.VMEM((2, seqs, half, width), F32),
                pltpu.VMEM((2, seqs, half, width), F32),
                pltpu.VMEM((seqs, seq_len, width), BF16),
                pltpu.VMEM((seqs, seq_len, width), BF16),
                dma((chips,)), dma((chips,)), dma((chips,)), dma((chips,)), dma((2,)), dma,
                dma((2, seqs)), dma((2, seqs)), dma((2, seqs)), dma((2, seqs)),
                dma((2, seqs, SUBS)), dma((2, seqs, SUBS)), dma((seqs, 2, SUBS)), dma((seqs, 2, SUBS)),
            ],
            compiler_params=pltpu.CompilerParams(collective_id=0, has_side_effects=True, vmem_limit_bytes=67000000),
            name='combine',
        )(table, expert_out[0], residual[0])

        def flat_t(w):
            return jnp.transpose(w[0], (1, 2, 0)).reshape(heads * head_dim, width)

        full = pl.BlockSpec((heads * head_dim, width), lambda i: (0, 0))
        seq_block = pl.BlockSpec((None, seq_len, width), lambda i: (i, 0, 0))
        result = pl.pallas_call(
            functools.partial(attn_kernel, head_dim),
            grid=(seqs,),
            out_shape=jax.ShapeDtypeStruct((seqs, seq_len, width), BF16),
            in_specs=[seq_block, pl.BlockSpec((1, width), lambda i: (0, 0)), full, full, full, full],
            out_specs=seq_block,
            scratch_shapes=[pltpu.VMEM((seq_len, heads * head_dim), BF16)] * 4,
            compiler_params=pltpu.CompilerParams(vmem_limit_bytes=60000000),
            name='attention',
        )(arrived, norm_scale, flat_t(w_query), flat_t(w_key), flat_t(w_value), w_out[0].reshape(heads * head_dim, width))
        return result[None]

    return jax.shard_map(body, mesh=mesh, in_specs=(token_spec, token_spec, token_spec, token_spec, token_spec, P('pp', None), weight_spec, weight_spec, weight_spec, weight_spec), out_specs=token_spec, check_vma=False)
```

```python
import functools
import math

import jax
import jax.numpy as jnp
from jax import lax
from jax.experimental import pallas as pl
from jax.experimental.pallas import tpu as pltpu
from jax.sharding import PartitionSpec as P

NORM_EPS = 1e-6
CORES = 2
LAG = 2
BLOCK = 128
F32 = jnp.float32
BF16 = jnp.bfloat16
MESH = pl.DeviceIdType.MESH
NT = (((1,), (1,)), ((), ()))
TN = (((0,), (0,)), ((), ()))


def stage_kernel(dims, ids_hbm, slots_hbm, gates_hbm, rows_hbm, resid_hbm, scale, wq_hbm, wk_hbm, wv_hbm, wo_hbm, out_hbm,
                 ids_in, slots_in, gates_in, own_rows, sib_rows, part, hop_in, dir_in, last_in, resid, y_buf, y_in,
                 meta_s, meta_r, sib_s, sib_r, own_sem, res_sem, w_sem, hop_s, hop_r, dir_s, dir_r, last_s, last_r,
                 y_s, y_r, z_sem):
    chips, stages, seqs, seq_len, cap, local, head_dim = dims
    blocks = seq_len // BLOCK
    half, sub = seq_len // 2, BLOCK // 2
    width = own_rows.shape[-1]
    quarter = width // local
    heads_step = quarter // head_dim
    ep = lax.axis_index('ep')
    stage = lax.axis_index('pp')
    chip, core = ep // CORES, ep % CORES

    def dev(delta):
        return {'ep': ((chip + delta) % chips) * CORES + core}

    sibling = {'ep': chip * CORES + 1 - core}
    up = {'pp': (stage + 1) % stages}
    down = {'pp': (stage + stages - 1) % stages}
    right, left = dev(1), dev(chips - 1)

    def owner_of(rel, which):
        return ((chip + rel) % chips) * CORES + which

    def remote(src, dst, ssem, rsem, device):
        return pltpu.make_async_remote_copy(src_ref=src, dst_ref=dst, send_sem=ssem, recv_sem=rsem, device_id=device, device_id_type=MESH)

    meta_pairs = ((ids_hbm, ids_in), (slots_hbm, slots_in), (gates_hbm, gates_in))

    def meta_copy(rel, i):
        src, dst = meta_pairs[i]
        return remote(src, dst.at[rel], meta_s.at[i, rel], meta_r.at[i, rel], dev(chips - rel))

    def meta_local(i):
        src, dst = meta_pairs[i]
        return pltpu.make_async_copy(src, dst.at[0], meta_r.at[i, 0])

    def sib_copy(rel, e):
        rows = pl.ds(pl.multiple_of(owner_of(rel, 1 - core) * cap, 8), cap)
        return remote(rows_hbm.at[e, rows], sib_rows.at[rel, e], sib_s.at[rel, e], sib_r.at[rel, e], sibling)

    def own_copy(rel, slot):
        rows = pl.ds(pl.multiple_of(owner_of(rel, core) * cap, 8), cap)
        return pltpu.make_async_copy(rows_hbm.at[:, rows], own_rows.at[slot], own_sem.at[slot])

    def weight_copy(i, j):
        src = (wq_hbm, wk_hbm, wv_hbm, wo_hbm)[i]
        return pltpu.make_async_copy(src.at[j * quarter:(j + 1) * quarter], sib_rows.at[i, j, 0:quarter], w_sem.at[i, j])

    def ring_copy(src, dst, ssem, rsem, way):
        return remote(src, dst, ssem, rsem, right if way == 0 else left)

    def hop_copy(way, s):
        return ring_copy(part.at[2, s, way], hop_in.at[way, s], hop_s.at[way, s], hop_r.at[way, s], way)

    def dir_copy(way, s):
        rel = 1 if way == 0 else chips - 1
        return ring_copy(part.at[rel, s, 1 - way], dir_in.at[way, s], dir_s.at[way, s], dir_r.at[way, s], way)

    def last_copy(way, s, u):
        rel = 1 if way == 0 else chips - 1
        span = pl.ds(u * sub, sub)
        return ring_copy(part.at[rel, s, way, span], last_in.at[way, s, span], last_s.at[way, s, u], last_r.at[way, s, u], way)

    def y_copy(s, u):
        span = pl.ds(u * BLOCK, BLOCK)
        return remote(y_buf.at[s, span], y_in.at[s, span], y_s.at[s, u], y_r.at[s, u], up)

    def z_copy(s, u):
        span = pl.ds(u * BLOCK, BLOCK)
        return pltpu.make_async_copy(y_buf.at[s, span], out_hbm.at[s, span], z_sem.at[s, u])

    def order(k):
        return (2 + 3 * k) % chips

    own_copy(2, 0).start()
    own_copy(order(1), 1).start()
    for i in range(3):
        meta_local(i).start()
    res_copy = pltpu.make_async_copy(resid_hbm, resid, res_sem)
    res_copy.start()

    barrier = pltpu.get_barrier_semaphore()
    peers = (sibling, right, left, dev(2), up, down)
    for peer in peers:
        pl.semaphore_signal(barrier, inc=1, device_id=peer, device_id_type=MESH)
    pl.semaphore_wait(barrier, len(peers))

    for rel in (2, 3, 1):
        for i in range(3):
            meta_copy(rel, i).start()
    for k in range(chips):
        for e in range(local):
            sib_copy(order(k), e).start()

    slot_iota = lax.broadcasted_iota(jnp.int32, (seq_len, cap), 1).astype(F32)
    expert_iota = lax.broadcasted_iota(jnp.int32, (CORES * local, seq_len), 0)

    def combine_block(rel, s, slot, before):
        ids, slots, gates = ids_in[rel, s], slots_in[rel, s], gates_in[rel, s]
        kept = slots >= 0
        local_slot = (slots - owner_of(rel, core) * cap).astype(F32)
        slot_rows = jnp.full((CORES * local, seq_len), -1.0, F32)
        gate_rows = jnp.zeros((CORES * local, seq_len), F32)
        for e in range(CORES * local):
            expert = (chip * CORES + (core if e < local else 1 - core)) * local + e % local
            match = jnp.logical_and(ids == expert, kept)
            slot_e = jnp.max(jnp.where(match, local_slot, -1.0), axis=0, keepdims=True)
            gate_e = jnp.sum(jnp.where(match, gates, 0.0), axis=0, keepdims=True)
            slot_rows = jnp.where(expert_iota == e, slot_e, slot_rows)
            gate_rows = jnp.where(expert_iota == e, gate_e, gate_rows)
        slot_cols, gate_cols = slot_rows.T, gate_rows.T
        for e in range(CORES * local):
            before(e)
            pick = jnp.where(slot_cols[:, e:e + 1] == slot_iota, 1.0, 0.0).astype(BF16)
            rows = own_rows[slot, e] if e < local else sib_rows[rel, e - local]
            term = gate_cols[:, e:e + 1] * jnp.dot(pick, rows, preferred_element_type=F32)
            for u in range(blocks):
                for w in range(2):
                    piece = term[u * BLOCK + w * sub:u * BLOCK + (w + 1) * sub]
                    if e == 0:
                        part[rel, s, w, u * sub:(u + 1) * sub] = piece
                    else:
                        part[rel, s, w, u * sub:(u + 1) * sub] += piece

    def first_wait(e):
        if e >= local:
            sib_copy(2, e - local).wait_recv()

    for i in range(3):
        meta_copy(2, i).wait_recv()
    own_copy(2, 0).wait()
    combine_block(2, 0, 0, first_wait)
    hop_copy(0, 0).start()
    hop_copy(1, 0).start()

    def combine_step(n, carry):
        k, s = n // seqs, n % seqs
        rel = order(k)
        slot = k % 2

        @pl.when(s == 0)
        def _():
            own_copy(rel, slot).wait()
            for e in range(local):
                sib_copy(rel, e).wait_recv()

            @pl.when(k < chips - 1)
            def _():
                own_copy(order(k + 1), 1 - slot).start()

            @pl.when(rel != 0)
            def _():
                for i in range(3):
                    meta_copy(rel, i).wait_recv()

            @pl.when(rel == 0)
            def _():
                for i in range(3):
                    meta_local(i).wait()

        combine_block(rel, s, slot, lambda e: None)

        @pl.when(rel == 2)
        def _():
            hop_copy(0, s).start()
            hop_copy(1, s).start()

        @pl.when(rel == 1)
        def _():
            dir_copy(0, s).start()

        @pl.when(rel == chips - 1)
        def _():
            dir_copy(1, s).start()

        return carry

    lax.fori_loop(1, chips * seqs, combine_step, 0)
    for i in range(4):
        for j in range(local):
            weight_copy(i, j).start()
    res_copy.wait()

    def relay_step(s, carry):
        for way in range(2):
            rel = 1 if way == 0 else chips - 1
            hop_copy(way, s).wait_recv()
            part[rel, s, way] += hop_in[way, s]
            for u in range(blocks):
                last_copy(way, s, u).start()
        return carry

    lax.fori_loop(0, seqs, relay_step, 0)
    for i in range(4):
        for j in range(local):
            weight_copy(i, j).wait()

    def merge_block(s, u):
        if u == 0:
            dir_copy(0, s).wait_recv()
            dir_copy(1, s).wait_recv()
        span = slice(u * sub, (u + 1) * sub)
        for w in range(2):
            last_copy(w, s, u).wait_recv()
            whole = slice(u * BLOCK + w * sub, u * BLOCK + (w + 1) * sub)
            total = resid[s, whole].astype(F32) + part[0, s, w, span] + dir_in[1 - w, s, span] + last_in[w, s, span]
            y_buf[s, whole] = total.astype(BF16)
        y_copy(s, u).start()

    factor = head_dim ** -0.5 * math.log2(math.e)
    causal = lax.broadcasted_iota(jnp.int32, (BLOCK, BLOCK), 0) <= lax.broadcasted_iota(jnp.int32, (BLOCK, BLOCK), 1)
    a_cols = slice(seq_len, seq_len + BLOCK)
    q_cols = slice(2 * seq_len, 2 * seq_len + BLOCK)

    def attend_block(s, u):
        y_copy(s, u).wait_recv()
        keys = (u + 1) * BLOCK
        here = slice(u * BLOCK, (u + 1) * BLOCK)
        y = y_in[s, here].astype(F32)
        inv_rms = lax.rsqrt(jnp.mean(y * y, axis=-1, keepdims=True) + NORM_EPS)
        x = (y * inv_rms * scale[...]).astype(BF16)
        for i, (plane, cols) in enumerate(((0, q_cols), (0, here), (1, here))):
            for j in range(local):
                heads = lax.dot_general(sib_rows[i, j, 0:quarter], x, NT, preferred_element_type=F32)
                own_rows[plane, j, 0:quarter, cols] = heads.astype(BF16)

        def heads_of(j, carry):
            spans = [slice(h * head_dim, (h + 1) * head_dim) for h in range(heads_step)]
            scores = [lax.dot_general(own_rows[0, j, r, 0:keys], own_rows[0, j, r, q_cols], TN, preferred_element_type=F32) for r in spans]
            probs, sums = [], []
            for t in scores:
                diag = jnp.where(causal, t[keys - BLOCK:], -1e30)
                t = diag if u == 0 else jnp.concatenate([t[:keys - BLOCK], diag], axis=0)
                t = jnp.exp2((t - jnp.max(t, axis=0, keepdims=True)) * factor)
                sums.append(jnp.sum(t, axis=0, keepdims=True))
                probs.append(t.astype(BF16))
            for r, t, total in zip(spans, probs, sums):
                mixed = jnp.dot(own_rows[1, j, r, 0:keys], t, preferred_element_type=F32)
                own_rows[1, j, r, a_cols] = (mixed / total).astype(BF16)
            return carry

        lax.fori_loop(0, local, heads_of, 0)
        proj = lax.dot_general(own_rows[1, 0, 0:quarter, a_cols], sib_rows[3, 0, 0:quarter], TN, preferred_element_type=F32)
        for j in range(1, local):
            proj += lax.dot_general(own_rows[1, j, 0:quarter, a_cols], sib_rows[3, j, 0:quarter], TN, preferred_element_type=F32)
        z = y_in[s, here].astype(F32) + proj.astype(BF16).astype(F32)
        y_copy(s, u).wait_send()
        y_buf[s, here] = z.astype(BF16)
        z_copy(s, u).start()

    def final_step(s, carry):
        for u in range(blocks):
            back = u - LAG
            past, at = (s, back) if back >= 0 else (s - 1, back + blocks)

            @pl.when(s < seqs)
            def _():
                merge_block(s, u)
                if back >= 0:
                    attend_block(past, at)

            if back < 0:
                @pl.when(s > 0)
                def _():
                    attend_block(past, at)
        return carry

    lax.fori_loop(0, seqs + 1, final_step, 0)

    def drain(s, carry):
        for way in range(2):
            hop_copy(way, s).wait_send()
            dir_copy(way, s).wait_send()
            for u in range(blocks):
                last_copy(way, s, u).wait_send()
        for u in range(blocks):
            z_copy(s, u).wait()
        return carry

    for rel in (2, 3, 1):
        for i in range(3):
            meta_copy(rel, i).wait_send()
    for k in range(chips):
        for e in range(local):
            sib_copy(order(k), e).wait_send()
    lax.fori_loop(0, seqs, drain, 0)


def solution(mesh):
    ep_size, pp_size = mesh.shape['ep'], mesh.shape['pp']
    chips = ep_size // CORES
    token_spec = P(('data', 'pp'), 'ep', None, None)
    weight_spec = P('pp', None, None, None)

    def body(expert_out, expert_ids, slot_ids, gate_vals, residual, norm_scale, w_query, w_key, w_value, w_out):
        local, capacity, width = expert_out.shape[1:]
        cap = capacity // ep_size
        seqs, seq_len, tops = expert_ids.shape[1:]
        half, blocks = seq_len // 2, seq_len // BLOCK
        heads, head_dim = w_query.shape[2:]
        routing = [jnp.swapaxes(a[0], 1, 2) for a in (expert_ids, slot_ids, gate_vals)]

        def flat_t(w):
            return jnp.transpose(w[0], (1, 2, 0)).reshape(heads * head_dim, width)

        dims = (chips, pp_size, seqs, seq_len, cap, local, head_dim)
        dma = pltpu.SemaphoreType.DMA
        any_spec = pl.BlockSpec(memory_space=pl.ANY)
        vmem_spec = pl.BlockSpec(memory_space=pltpu.VMEM)
        result = pl.pallas_call(
            functools.partial(stage_kernel, dims),
            out_shape=jax.ShapeDtypeStruct((seqs, seq_len, width), BF16),
            in_specs=[any_spec] * 5 + [vmem_spec] + [any_spec] * 4,
            out_specs=any_spec,
            scratch_shapes=[
                pltpu.VMEM((chips, seqs, tops, seq_len), jnp.int32),
                pltpu.VMEM((chips, seqs, tops, seq_len), jnp.int32),
                pltpu.VMEM((chips, seqs, tops, seq_len), F32),
                pltpu.VMEM((2, local, cap, width), BF16),
                pltpu.VMEM((chips, local, cap, width), BF16),
                pltpu.VMEM((chips, seqs, 2, half, width), F32),
                pltpu.VMEM((2, seqs, half, width), F32),
                pltpu.VMEM((2, seqs, half, width), F32),
                pltpu.VMEM((2, seqs, half, width), F32),
                pltpu.VMEM((seqs, seq_len, width), BF16),
                pltpu.VMEM((seqs, seq_len, width), BF16),
                pltpu.VMEM((seqs, seq_len, width), BF16),
                dma((3, chips)), dma((3, chips)), dma((chips, local)), dma((chips, local)), dma((2,)), dma, dma((4, local)),
                dma((2, seqs)), dma((2, seqs)), dma((2, seqs)), dma((2, seqs)),
                dma((2, seqs, blocks)), dma((2, seqs, blocks)), dma((seqs, blocks)), dma((seqs, blocks)), dma((seqs, blocks)),
            ],
            compiler_params=pltpu.CompilerParams(collective_id=0, has_side_effects=True, vmem_limit_bytes=67000000),
            name='stage',
        )(*routing, expert_out[0], residual[0], norm_scale, flat_t(w_query), flat_t(w_key), flat_t(w_value),
          w_out[0].reshape(heads * head_dim, width))
        return result[None]

    return jax.shard_map(body, mesh=mesh, in_specs=(token_spec, token_spec, token_spec, token_spec, token_spec, P('pp', None), weight_spec, weight_spec, weight_spec, weight_spec), out_specs=token_spec, check_vma=False)
```

```python
import functools
import math

import jax
import jax.numpy as jnp
from jax import lax
from jax.experimental import pallas as pl
from jax.experimental.pallas import tpu as pltpu
from jax.sharding import PartitionSpec as P

NORM_EPS = 1e-6
NONE = -256.0
CORES = 2
BLOCK = 128
PIECES = (1, 2, 4)
STRIPS = 4
PAIRS = 4
F32 = jnp.float32
BF16 = jnp.bfloat16
MESH = pl.DeviceIdType.MESH
NT = (((1,), (1,)), ((), ()))
TN = (((0,), (0,)), ((), ()))


def stage_kernel(dims, ids_hbm, slots_hbm, gates_hbm, rows_hbm, resid_hbm, scale, wq_hbm, wk_hbm, wv_hbm, wo_hbm, out_ref,
                 ids_in, slots_in, gates_in, slot_out, gate_out, slot_in, gate_in, own_rows, sib_rows, part, hop_in, dir_in, last_in, resid, y_buf, y_in,
                 in_sem, meta_s, meta_r, sib_s, sib_r, own_sem, res_sem, w_sem, hop_s, hop_r, dir_s, dir_r, last_s, last_r,
                 y_s, y_r):
    chips, stages, seqs, seq_len, cap, local, head_dim = dims
    blocks = seq_len // BLOCK
    half, sub = seq_len // 2, BLOCK // 2
    strip = sub // STRIPS
    width = own_rows.shape[-1]
    quarter = width // local
    heads_step = quarter // head_dim
    ep = lax.axis_index('ep')
    stage = lax.axis_index('pp')
    chip, core = ep // CORES, ep % CORES

    def dev(delta):
        return {'ep': ((chip + delta) % chips) * CORES + core}

    sibling = {'ep': chip * CORES + 1 - core}
    up = {'pp': (stage + 1) % stages}
    down = {'pp': (stage + stages - 1) % stages}
    right, left = dev(1), dev(chips - 1)

    def owner_of(rel, which):
        return ((chip + rel) % chips) * CORES + which

    def remote(src, dst, ssem, rsem, device):
        return pltpu.make_async_remote_copy(src_ref=src, dst_ref=dst, send_sem=ssem, recv_sem=rsem, device_id=device, device_id_type=MESH)

    def in_copy(i):
        src, dst = ((ids_hbm, ids_in), (slots_hbm, slots_in), (gates_hbm, gates_in))[i]
        return pltpu.make_async_copy(src, dst, in_sem.at[i])

    def meta_copy(rel, s, i):
        src, dst = ((slot_out, slot_in), (gate_out, gate_in))[i]
        return remote(src.at[rel, s], dst.at[rel, s], meta_s.at[i, rel, s], meta_r.at[i, rel, s], dev(chips - rel))

    def sib_copy(rel, e):
        rows = pl.ds(pl.multiple_of(owner_of(rel, 1 - core) * cap, 8), cap)
        return remote(rows_hbm.at[e, rows], sib_rows.at[rel, e], sib_s.at[rel, e], sib_r.at[rel, e], sibling)

    def own_copy(rel, slot):
        rows = pl.ds(pl.multiple_of(owner_of(rel, core) * cap, 8), cap)
        return pltpu.make_async_copy(rows_hbm.at[:, rows], own_rows.at[slot], own_sem.at[slot])

    def weight_copy(i, j):
        src = (wq_hbm, wk_hbm, wv_hbm, wo_hbm)[i]
        return pltpu.make_async_copy(src.at[j * quarter:(j + 1) * quarter], sib_rows.at[i, j, 0:quarter], w_sem.at[i, j])

    def ring_copy(src, dst, ssem, rsem, way):
        return remote(src, dst, ssem, rsem, right if way == 0 else left)

    def hop_copy(way, s):
        return ring_copy(part.at[2, s, way], hop_in.at[way, s], hop_s.at[way, s], hop_r.at[way, s], way)

    def dir_copy(way, s, u):
        rel = 1 if way == 0 else chips - 1
        span = pl.ds(u * sub, sub)
        return ring_copy(part.at[rel, s, 1 - way, span], dir_in.at[way, s, span], dir_s.at[way, s, u], dir_r.at[way, s, u], way)

    def last_copy(way, s, u, p):
        rel = 1 if way == 0 else chips - 1
        rows, i = sub // PIECES[u], sum(PIECES[:u]) + p
        span = pl.ds(u * sub + p * rows, rows)
        return ring_copy(part.at[rel, s, way, span], last_in.at[way, s, span], last_s.at[way, s, i], last_r.at[way, s, i], way)

    def y_copy(s, u, p):
        rows, i = BLOCK // PIECES[u], sum(PIECES[:u]) + p
        span = pl.ds(u * BLOCK + p * rows, rows)
        return remote(y_buf.at[s, span], y_in.at[s, span], y_s.at[s, i], y_r.at[s, i], up)

    def order(k):
        return (2 + 3 * (k + k // 2 - 2 * (k // 3))) % chips

    for i in range(3):
        in_copy(i).start()
    own_copy(2, 0).start()
    own_copy(1, 1).start()
    res_copy = pltpu.make_async_copy(resid_hbm, resid, res_sem)
    res_copy.start()

    barrier = pltpu.get_barrier_semaphore()
    peers = (sibling, right, left, dev(2), up, down)
    for peer in peers:
        pl.semaphore_signal(barrier, inc=1, device_id=peer, device_id_type=MESH)

    for i in range(3):
        in_copy(i).wait()
    expert_iota = lax.broadcasted_iota(jnp.int32, (CORES * local, seq_len), 0)

    def table_step(s, carry):
        ids, gates = ids_in[s], gates_in[s]
        kept = slots_in[s] >= 0
        code = (slots_in[s] - (ep * cap + cap // 2)).astype(F32)
        for rel in (2, 1, 0, 3):
            target = (chip + chips - rel) % chips
            slot_rows = jnp.full((CORES * local, seq_len), NONE, F32)
            gate_rows = jnp.zeros((CORES * local, seq_len), F32)
            for e in range(CORES * local):
                expert = (target * CORES + (core if e < local else 1 - core)) * local + e % local
                match = jnp.logical_and(ids == expert, kept)
                slot_e = jnp.max(jnp.where(match, code, NONE), axis=0, keepdims=True)
                gate_e = jnp.sum(jnp.where(match, gates, 0.0), axis=0, keepdims=True)
                slot_rows = jnp.where(expert_iota == e, slot_e, slot_rows)
                gate_rows = jnp.where(expert_iota == e, gate_e, gate_rows)
            slot_to, gate_to = (slot_in, gate_in) if rel == 0 else (slot_out, gate_out)
            slot_to[rel, s] = slot_rows.astype(BF16)
            gate_to[rel, s] = gate_rows
        return carry

    lax.fori_loop(0, seqs, table_step, 0)
    pl.semaphore_wait(barrier, len(peers))

    for s in range(seqs):
        for rel in (2, 1, 3):
            for i in range(2):
                meta_copy(rel, s, i).start()
    for k in range(chips):
        for e in range(local):
            sib_copy(order(k), e).start()

    slot_iota = (lax.broadcasted_iota(jnp.int32, (seq_len, cap), 1) - cap // 2).astype(F32)

    def combine_block(rel, s, slot, before):
        slot_cols, gate_cols = slot_in[rel, s].astype(F32).T, gate_in[rel, s].T
        for e in range(CORES * local):
            before(e)
            pick = jnp.where(slot_cols[:, e:e + 1] == slot_iota, 1.0, 0.0).astype(BF16)
            rows = own_rows[slot, e] if e < local else sib_rows[rel, e - local]
            term = gate_cols[:, e:e + 1] * jnp.dot(pick, rows, preferred_element_type=F32)
            for i in range(half // strip):
                for w in range(2):
                    piece = term[(2 * i + w) * strip:(2 * i + w + 1) * strip]
                    if e == 0:
                        part[rel, s, w, i * strip:(i + 1) * strip] = piece
                    else:
                        part[rel, s, w, i * strip:(i + 1) * strip] += piece

    def first_wait(e):
        if e >= local:
            sib_copy(2, e - local).wait_recv()

    own_copy(2, 0).wait()
    for i in range(2):
        meta_copy(2, 0, i).wait_recv()
    combine_block(2, 0, 0, first_wait)
    hop_copy(0, 0).start()
    hop_copy(1, 0).start()

    def relay(s, last):
        for way in range(2):
            rel = 1 if way == 0 else chips - 1
            hop_copy(way, s).wait_recv()
            part[rel, s, way] += hop_in[way, s]
        for u in range(blocks):
            for way in range(2):
                if last:
                    dir_copy(way, s, u).start()
                for p in range(PIECES[u]):
                    last_copy(way, s, u, p).start()

    def combine_step(n, carry):
        s, k = n // chips, n % chips
        rel = order(k)
        slot = n % 2

        @pl.when(n < seqs * chips - 1)
        def _():
            own_copy(order((n + 1) % chips), 1 - slot).start()

        @pl.when(n == chips + 1)
        def _():
            relay(0, False)

        own_copy(rel, slot).wait()

        @pl.when(s == 0)
        def _():
            for e in range(local):
                sib_copy(rel, e).wait_recv()

        @pl.when(rel != 0)
        def _():
            for i in range(2):
                meta_copy(rel, s, i).wait_recv()

        combine_block(rel, s, slot, lambda e: None)

        @pl.when(rel == 2)
        def _():
            hop_copy(0, s).start()
            hop_copy(1, s).start()

        for way, ready in ((0, 1), (1, chips - 1)):
            @pl.when(jnp.logical_and(rel == ready, s < seqs - 1))
            def _():
                for u in range(blocks):
                    dir_copy(way, s, u).start()

        return carry

    lax.fori_loop(1, chips * seqs, combine_step, 0)
    for i in range(4):
        for j in range(local):
            weight_copy(i, j).start()
    res_copy.wait()
    relay(1, False)
    for i in range(4):
        for j in range(local):
            weight_copy(i, j).wait()

    def merge_block(s, u):
        dir_copy(0, s, u).wait_recv()
        dir_copy(1, s, u).wait_recv()
        each = STRIPS // PIECES[u]
        for p in range(PIECES[u]):
            for w in range(2):
                last_copy(w, s, u, p).wait_recv()
            for i in range(u * STRIPS + p * each, u * STRIPS + (p + 1) * each):
                span = slice(i * strip, (i + 1) * strip)
                for w in range(2):
                    whole = slice((2 * i + w) * strip, (2 * i + w + 1) * strip)
                    total = resid[s, whole].astype(F32) + part[0, s, w, span] + dir_in[1 - w, s, span] + last_in[w, s, span]
                    y_buf[s, whole] = total.astype(BF16)
            y_copy(s, u, p).start()

    factor = head_dim ** -0.5 * math.log2(math.e)
    causal = lax.broadcasted_iota(jnp.int32, (BLOCK, 2 * BLOCK), 0) <= lax.broadcasted_iota(jnp.int32, (BLOCK, 2 * BLOCK), 1) % BLOCK
    gap = jnp.zeros((head_dim, BLOCK), BF16)
    a_cols = slice(seq_len, seq_len + BLOCK)
    q_cols = slice(2 * seq_len, 2 * seq_len + BLOCK)

    def attend_block(s, u):
        for p in range(PIECES[u]):
            y_copy(s, u, p).wait_recv()
        keys = (u + 1) * BLOCK
        here = slice(u * BLOCK, (u + 1) * BLOCK)
        y = y_in[s, here].astype(F32)
        inv_rms = lax.rsqrt(jnp.mean(y * y, axis=-1, keepdims=True) + NORM_EPS)
        x = (y * inv_rms * scale[...]).astype(BF16)
        for i, (plane, cols) in enumerate(((0, q_cols), (0, here), (1, here))):
            for j in range(local):
                heads = lax.dot_general(sib_rows[i, j, 0:quarter], x, NT, preferred_element_type=F32)
                own_rows[plane, j, 0:quarter, cols] = heads.astype(BF16)

        def heads_of(step, carry):
            places = []
            for i in range(PAIRS):
                first = i % (heads_step // 2) * 2 * head_dim
                places.append((step * (PAIRS * 2 // heads_step) + i // (heads_step // 2), first))
            scores = []
            for j, first in places:
                q_one = own_rows[0, j, first:first + head_dim, q_cols]
                q_two = own_rows[0, j, first + head_dim:first + 2 * head_dim, q_cols]
                both = jnp.concatenate([jnp.concatenate([q_one, gap], axis=1), jnp.concatenate([gap, q_two], axis=1)], axis=0)
                k_pair = own_rows[0, j, first:first + 2 * head_dim, 0:keys]
                scores.append(lax.dot_general(k_pair, both, TN, preferred_element_type=F32))
            probs, sums = [], []
            for t in scores:
                diag = jnp.where(causal, t[keys - BLOCK:], -1e30)
                t = diag if u == 0 else jnp.concatenate([t[:keys - BLOCK], diag], axis=0)
                t = jnp.exp2((t - jnp.max(t, axis=0, keepdims=True)) * factor)
                sums.append(jnp.sum(t, axis=0, keepdims=True))
                probs.append(t.astype(BF16))
            for (j, first), t, total in zip(places, probs, sums):
                mixed = jnp.dot(own_rows[1, j, first:first + 2 * head_dim, 0:keys], t, preferred_element_type=F32)
                for h in range(2):
                    rows, cols = slice(h * head_dim, (h + 1) * head_dim), slice(h * BLOCK, (h + 1) * BLOCK)
                    own_rows[1, j, first + rows.start:first + rows.stop, a_cols] = (mixed[rows, cols] / total[:, cols]).astype(BF16)
            return carry

        lax.fori_loop(0, width // head_dim // (2 * PAIRS), heads_of, 0)
        proj = lax.dot_general(own_rows[1, 0, 0:quarter, a_cols], sib_rows[3, 0, 0:quarter], TN, preferred_element_type=F32)
        for j in range(1, local):
            proj += lax.dot_general(own_rows[1, j, 0:quarter, a_cols], sib_rows[3, j, 0:quarter], TN, preferred_element_type=F32)
        z = y_in[s, here].astype(F32) + proj.astype(BF16).astype(F32)
        out_ref[s, here] = z.astype(BF16)

    def final_step(s, carry):
        @pl.when(s == seqs - 2)
        def _():
            relay(seqs - 1, True)

        for u in range(blocks):
            merge_block(s, u)
            if u < blocks - 1:
                @pl.when(s == seqs - 1)
                def _():
                    attend_block(s, u)

        @pl.when(s < seqs - 1)
        def _():
            for u in range(blocks - 1):
                attend_block(s, u)

        attend_block(s, blocks - 1)
        return carry

    lax.fori_loop(0, seqs, final_step, 0)

    def drain(s, carry):
        for way in range(2):
            hop_copy(way, s).wait_send()
            for u in range(blocks):
                dir_copy(way, s, u).wait_send()
                for p in range(PIECES[u]):
                    last_copy(way, s, u, p).wait_send()
        for u in range(blocks):
            for p in range(PIECES[u]):
                y_copy(s, u, p).wait_send()
        return carry

    for rel in (2, 1, 3):
        for s in range(seqs):
            for i in range(2):
                meta_copy(rel, s, i).wait_send()
    for k in range(chips):
        for e in range(local):
            sib_copy(order(k), e).wait_send()
    lax.fori_loop(0, seqs, drain, 0)


def solution(mesh):
    ep_size, pp_size = mesh.shape['ep'], mesh.shape['pp']
    chips = ep_size // CORES
    token_spec = P(('data', 'pp'), 'ep', None, None)
    weight_spec = P('pp', None, None, None)

    def body(expert_out, expert_ids, slot_ids, gate_vals, residual, norm_scale, w_query, w_key, w_value, w_out):
        local, capacity, width = expert_out.shape[1:]
        cap = capacity // ep_size
        seqs, seq_len, tops = expert_ids.shape[1:]
        half, blocks, pieces = seq_len // 2, seq_len // BLOCK, sum(PIECES)
        assert len(PIECES) == blocks and cap // 2 < -NONE
        heads, head_dim = w_query.shape[2:]
        routing = [jnp.swapaxes(a[0], 1, 2) for a in (expert_ids, slot_ids, gate_vals)]

        def flat_t(w):
            return jnp.transpose(w[0], (1, 2, 0)).reshape(heads * head_dim, width)

        dims = (chips, pp_size, seqs, seq_len, cap, local, head_dim)
        dma = pltpu.SemaphoreType.DMA
        any_spec = pl.BlockSpec(memory_space=pl.ANY)
        vmem_spec = pl.BlockSpec(memory_space=pltpu.VMEM)
        result = pl.pallas_call(
            functools.partial(stage_kernel, dims),
            out_shape=pltpu.VMEM((seqs, seq_len, width), BF16),
            in_specs=[any_spec] * 5 + [vmem_spec] + [any_spec] * 4,
            out_specs=vmem_spec,
            scratch_shapes=[
                pltpu.VMEM((seqs, tops, seq_len), jnp.int32),
                pltpu.VMEM((seqs, tops, seq_len), jnp.int32),
                pltpu.VMEM((seqs, tops, seq_len), F32),
                pltpu.VMEM((chips, seqs, CORES * local, seq_len), BF16),
                pltpu.VMEM((chips, seqs, CORES * local, seq_len), F32),
                pltpu.VMEM((chips, seqs, CORES * local, seq_len), BF16),
                pltpu.VMEM((chips, seqs, CORES * local, seq_len), F32),
                pltpu.VMEM((2, local, cap, width), BF16),
                pltpu.VMEM((chips, local, cap, width), BF16),
                pltpu.VMEM((chips, seqs, 2, half, width), F32),
                pltpu.VMEM((2, seqs, half, width), F32),
                pltpu.VMEM((2, seqs, half, width), F32),
                pltpu.VMEM((2, seqs, half, width), F32),
                pltpu.VMEM((seqs, seq_len, width), BF16),
                pltpu.VMEM((seqs, seq_len, width), BF16),
                pltpu.VMEM((seqs, seq_len, width), BF16),
                dma((3,)), dma((2, chips, seqs)), dma((2, chips, seqs)), dma((chips, local)), dma((chips, local)), dma((2,)), dma, dma((4, local)),
                dma((2, seqs)), dma((2, seqs)), dma((2, seqs, blocks)), dma((2, seqs, blocks)),
                dma((2, seqs, pieces)), dma((2, seqs, pieces)), dma((seqs, pieces)), dma((seqs, pieces)),
            ],
            compiler_params=pltpu.CompilerParams(collective_id=0, has_side_effects=True, vmem_limit_bytes=64200000),
            name='stage',
        )(*routing, expert_out[0], residual[0], norm_scale, flat_t(w_query), flat_t(w_key), flat_t(w_value),
          w_out[0].reshape(heads * head_dim, width))
        return result[None]

    return jax.shard_map(body, mesh=mesh, in_specs=(token_spec, token_spec, token_spec, token_spec, token_spec, P('pp', None), weight_spec, weight_spec, weight_spec, weight_spec), out_specs=token_spec, check_vma=False)
```

```python
import functools
import math

import jax
import jax.numpy as jnp
from jax import lax
from jax.experimental import pallas as pl
from jax.experimental.pallas import tpu as pltpu
from jax.sharding import PartitionSpec as P

NORM_EPS = 1e-6
NONE = -256.0
CORES = 2
BLOCK = 128
PIECES = (1, 2, 4)
STRIPS = 4
PAIRS = 8
F32 = jnp.float32
BF16 = jnp.bfloat16
MESH = pl.DeviceIdType.MESH
NT = (((1,), (1,)), ((), ()))
TN = (((0,), (0,)), ((), ()))


def stage_kernel(dims, ids_hbm, slots_hbm, gates_hbm, rows_hbm, resid_hbm, scale, wq_hbm, wk_hbm, wv_hbm, wo_hbm, out_ref,
                 ids_in, slots_in, gates_in, slot_out, gate_out, slot_in, gate_in, own_rows, sib_rows, part, hop_in, dir_in, last_in, resid, y_buf, y_in,
                 in_sem, meta_s, meta_r, sib_s, sib_r, own_sem, res_sem, w_sem, hop_s, hop_r, dir_s, dir_r, last_s, last_r,
                 y_s, y_r):
    chips, stages, seqs, seq_len, cap, local, head_dim = dims
    blocks = seq_len // BLOCK
    half, sub = seq_len // 2, BLOCK // 2
    strip = sub // STRIPS
    width = own_rows.shape[-1]
    quarter = width // local
    heads_step = quarter // head_dim
    ep = lax.axis_index('ep')
    stage = lax.axis_index('pp')
    chip, core = ep // CORES, ep % CORES

    def dev(delta):
        return {'ep': ((chip + delta) % chips) * CORES + core}

    sibling = {'ep': chip * CORES + 1 - core}
    up = {'pp': (stage + 1) % stages}
    down = {'pp': (stage + stages - 1) % stages}
    right, left = dev(1), dev(chips - 1)

    def owner_of(rel, which):
        return ((chip + rel) % chips) * CORES + which

    def remote(src, dst, ssem, rsem, device):
        return pltpu.make_async_remote_copy(src_ref=src, dst_ref=dst, send_sem=ssem, recv_sem=rsem, device_id=device, device_id_type=MESH)

    def in_copy(i):
        src, dst = ((ids_hbm, ids_in), (slots_hbm, slots_in), (gates_hbm, gates_in))[i]
        return pltpu.make_async_copy(src, dst, in_sem.at[i])

    def meta_copy(rel, s, i):
        src, dst = ((slot_out, slot_in), (gate_out, gate_in))[i]
        return remote(src.at[rel, s], dst.at[rel, s], meta_s.at[i, rel, s], meta_r.at[i, rel, s], dev(chips - rel))

    def sib_copy(rel, e):
        rows = pl.ds(pl.multiple_of(owner_of(rel, 1 - core) * cap, 8), cap)
        return remote(rows_hbm.at[e, rows], sib_rows.at[rel, e], sib_s.at[rel, e], sib_r.at[rel, e], sibling)

    def own_copy(rel, slot):
        rows = pl.ds(pl.multiple_of(owner_of(rel, core) * cap, 8), cap)
        return pltpu.make_async_copy(rows_hbm.at[:, rows], own_rows.at[slot], own_sem.at[slot])

    def weight_copy(i, j):
        src = (wq_hbm, wk_hbm, wv_hbm, wo_hbm)[i]
        return pltpu.make_async_copy(src.at[j * quarter:(j + 1) * quarter], sib_rows.at[i, j, 0:quarter], w_sem.at[i, j])

    def ring_copy(src, dst, ssem, rsem, way):
        return remote(src, dst, ssem, rsem, right if way == 0 else left)

    def hop_copy(way, s):
        return ring_copy(part.at[2, s, way], hop_in.at[way, s], hop_s.at[way, s], hop_r.at[way, s], way)

    def dir_copy(way, s, u, last):
        rel = 1 if way == 0 else chips - 1
        span = pl.ds(u * sub, sub) if last else pl.ds(0, half)
        return ring_copy(part.at[rel, s, 1 - way, span], dir_in.at[way, s, span], dir_s.at[way, s, u], dir_r.at[way, s, u], way)

    def last_copy(way, s, u, p, last):
        rel = 1 if way == 0 else chips - 1
        rows, i = sub // pieces(u, last), sum(PIECES[:u]) + p
        span = pl.ds(u * sub + p * rows, rows)
        return ring_copy(part.at[rel, s, way, span], last_in.at[way, s, span], last_s.at[way, s, i], last_r.at[way, s, i], way)

    def y_copy(s, u, p, last):
        rows, i = BLOCK // pieces(u, last), sum(PIECES[:u]) + p
        span = pl.ds(u * BLOCK + p * rows, rows)
        return remote(y_buf.at[s, span], y_in.at[s, span], y_s.at[s, i], y_r.at[s, i], up)

    def pieces(u, last):
        return PIECES[u] if last else 1

    def dir_blocks(last):
        return blocks if last else 1

    def order(k):
        return (2 + 3 * (k + k // 2 - 2 * (k // 3))) % chips

    for i in range(3):
        in_copy(i).start()
    own_copy(2, 0).start()
    own_copy(1, 1).start()
    res_copy = pltpu.make_async_copy(resid_hbm, resid, res_sem)
    res_copy.start()

    barrier = pltpu.get_barrier_semaphore()
    peers = (sibling, right, left, dev(2), up, down)
    for peer in peers:
        pl.semaphore_signal(barrier, inc=1, device_id=peer, device_id_type=MESH)

    for i in range(3):
        in_copy(i).wait()
    expert_iota = lax.broadcasted_iota(jnp.int32, (CORES * local, seq_len), 0)

    def table_step(s, carry):
        ids, gates = ids_in[s], gates_in[s]
        kept = slots_in[s] >= 0
        code = (slots_in[s] - (ep * cap + cap // 2)).astype(F32)
        for rel in (2, 1, 0, 3):
            target = (chip + chips - rel) % chips
            slot_rows = jnp.full((CORES * local, seq_len), NONE, F32)
            gate_rows = jnp.zeros((CORES * local, seq_len), F32)
            for e in range(CORES * local):
                expert = (target * CORES + (core if e < local else 1 - core)) * local + e % local
                match = jnp.logical_and(ids == expert, kept)
                slot_e = jnp.max(jnp.where(match, code, NONE), axis=0, keepdims=True)
                gate_e = jnp.sum(jnp.where(match, gates, 0.0), axis=0, keepdims=True)
                slot_rows = jnp.where(expert_iota == e, slot_e, slot_rows)
                gate_rows = jnp.where(expert_iota == e, gate_e, gate_rows)
            slot_to, gate_to = (slot_in, gate_in) if rel == 0 else (slot_out, gate_out)
            slot_to[rel, s] = slot_rows.astype(BF16)
            gate_to[rel, s] = gate_rows
        return carry

    lax.fori_loop(0, seqs, table_step, 0)
    pl.semaphore_wait(barrier, len(peers))

    for s in range(seqs):
        for rel in (2, 1, 3):
            for i in range(2):
                meta_copy(rel, s, i).start()
    for k in range(chips):
        for e in range(local):
            sib_copy(order(k), e).start()

    slot_iota = (lax.broadcasted_iota(jnp.int32, (seq_len, cap), 1) - cap // 2).astype(F32)

    def combine_block(rel, s, slot, before):
        slot_cols, gate_cols = slot_in[rel, s].astype(F32).T, gate_in[rel, s].T
        for e in range(CORES * local):
            before(e)
            pick = jnp.where(slot_cols[:, e:e + 1] == slot_iota, 1.0, 0.0).astype(BF16)
            rows = own_rows[slot, e] if e < local else sib_rows[rel, e - local]
            term = gate_cols[:, e:e + 1] * jnp.dot(pick, rows, preferred_element_type=F32)
            for i in range(half // strip):
                for w in range(2):
                    piece = term[(2 * i + w) * strip:(2 * i + w + 1) * strip]
                    if e == 0:
                        part[rel, s, w, i * strip:(i + 1) * strip] = piece
                    else:
                        part[rel, s, w, i * strip:(i + 1) * strip] += piece

    def first_wait(e):
        if e >= local:
            sib_copy(2, e - local).wait_recv()

    own_copy(2, 0).wait()
    for i in range(2):
        meta_copy(2, 0, i).wait_recv()
    combine_block(2, 0, 0, first_wait)
    hop_copy(0, 0).start()
    hop_copy(1, 0).start()

    def relay(s, last):
        for way in range(2):
            rel = 1 if way == 0 else chips - 1
            hop_copy(way, s).wait_recv()
            part[rel, s, way] += hop_in[way, s]
        for u in range(blocks):
            for way in range(2):
                if last:
                    dir_copy(way, s, u, True).start()
                for p in range(pieces(u, last)):
                    last_copy(way, s, u, p, last).start()

    def combine_step(n, carry):
        s, k = n // chips, n % chips
        rel = order(k)
        slot = n % 2

        @pl.when(n < seqs * chips - 1)
        def _():
            own_copy(order((n + 1) % chips), 1 - slot).start()

        @pl.when(n == chips + 1)
        def _():
            relay(0, False)

        own_copy(rel, slot).wait()

        @pl.when(s == 0)
        def _():
            for e in range(local):
                sib_copy(rel, e).wait_recv()

        @pl.when(rel != 0)
        def _():
            for i in range(2):
                meta_copy(rel, s, i).wait_recv()

        combine_block(rel, s, slot, lambda e: None)

        @pl.when(rel == 2)
        def _():
            hop_copy(0, s).start()
            hop_copy(1, s).start()

        for way, ready in ((0, 1), (1, chips - 1)):
            @pl.when(jnp.logical_and(rel == ready, s < seqs - 1))
            def _():
                dir_copy(way, s, 0, False).start()

        return carry

    lax.fori_loop(1, chips * seqs, combine_step, 0)
    for i in range(4):
        for j in range(local):
            weight_copy(i, j).start()
    res_copy.wait()
    relay(1, False)
    for i in range(4):
        for j in range(local):
            weight_copy(i, j).wait()

    def merge_block(s, u, last):
        if u < dir_blocks(last):
            dir_copy(0, s, u, last).wait_recv()
            dir_copy(1, s, u, last).wait_recv()
        each = STRIPS // pieces(u, last)
        for p in range(pieces(u, last)):
            for w in range(2):
                last_copy(w, s, u, p, last).wait_recv()
            for i in range(u * STRIPS + p * each, u * STRIPS + (p + 1) * each):
                span = slice(i * strip, (i + 1) * strip)
                for w in range(2):
                    whole = slice((2 * i + w) * strip, (2 * i + w + 1) * strip)
                    total = resid[s, whole].astype(F32) + part[0, s, w, span] + dir_in[1 - w, s, span] + last_in[w, s, span]
                    y_buf[s, whole] = total.astype(BF16)
            y_copy(s, u, p, last).start()

    factor = head_dim ** -0.5 * math.log2(math.e)
    causal = lax.broadcasted_iota(jnp.int32, (BLOCK, 2 * BLOCK), 0) <= lax.broadcasted_iota(jnp.int32, (BLOCK, 2 * BLOCK), 1) % BLOCK
    gap = jnp.zeros((head_dim, BLOCK), BF16)
    a_cols = slice(seq_len, seq_len + BLOCK)
    q_cols = slice(2 * seq_len, 2 * seq_len + BLOCK)

    def attend_block(s, u, last):
        for p in range(pieces(u, last)):
            y_copy(s, u, p, last).wait_recv()
        keys = (u + 1) * BLOCK
        here = slice(u * BLOCK, (u + 1) * BLOCK)
        y = y_in[s, here].astype(F32)
        inv_rms = lax.rsqrt(jnp.mean(y * y, axis=-1, keepdims=True) + NORM_EPS)
        x = (y * inv_rms * scale[...]).astype(BF16)
        for i, (plane, cols) in enumerate(((0, q_cols), (0, here), (1, here))):
            for j in range(local):
                heads = lax.dot_general(sib_rows[i, j, 0:quarter], x, NT, preferred_element_type=F32)
                own_rows[plane, j, 0:quarter, cols] = heads.astype(BF16)

        def heads_of(step, carry):
            places = []
            for i in range(PAIRS):
                first = i % (heads_step // 2) * 2 * head_dim
                places.append((step * (PAIRS * 2 // heads_step) + i // (heads_step // 2), first))
            scores = []
            for j, first in places:
                q_one = own_rows[0, j, first:first + head_dim, q_cols]
                q_two = own_rows[0, j, first + head_dim:first + 2 * head_dim, q_cols]
                both = jnp.concatenate([jnp.concatenate([q_one, gap], axis=1), jnp.concatenate([gap, q_two], axis=1)], axis=0)
                k_pair = own_rows[0, j, first:first + 2 * head_dim, 0:keys]
                scores.append(lax.dot_general(k_pair, both, TN, preferred_element_type=F32))
            probs, sums = [], []
            for t in scores:
                diag = jnp.where(causal, t[keys - BLOCK:], -1e30)
                t = diag if u == 0 else jnp.concatenate([t[:keys - BLOCK], diag], axis=0)
                t = jnp.exp2((t - jnp.max(t, axis=0, keepdims=True)) * factor)
                sums.append(jnp.sum(t, axis=0, keepdims=True))
                probs.append(t.astype(BF16))
            for (j, first), t, total in zip(places, probs, sums):
                mixed = jnp.dot(own_rows[1, j, first:first + 2 * head_dim, 0:keys], t, preferred_element_type=F32)
                for h in range(2):
                    rows, cols = slice(h * head_dim, (h + 1) * head_dim), slice(h * BLOCK, (h + 1) * BLOCK)
                    own_rows[1, j, first + rows.start:first + rows.stop, a_cols] = (mixed[rows, cols] / total[:, cols]).astype(BF16)
            return carry

        lax.fori_loop(0, width // head_dim // (2 * PAIRS), heads_of, 0)
        proj = lax.dot_general(own_rows[1, 0, 0:quarter, a_cols], sib_rows[3, 0, 0:quarter], TN, preferred_element_type=F32)
        for j in range(1, local):
            proj += lax.dot_general(own_rows[1, j, 0:quarter, a_cols], sib_rows[3, j, 0:quarter], TN, preferred_element_type=F32)
        z = y_in[s, here].astype(F32) + proj.astype(BF16).astype(F32)
        out_ref[s, here] = z.astype(BF16)

    def final_step(s, carry):
        @pl.when(s == seqs - 2)
        def _():
            relay(seqs - 1, True)

        for u in range(blocks):
            merge_block(s, u, False)
        for u in range(blocks):
            attend_block(s, u, False)
        return carry

    lax.fori_loop(0, seqs - 1, final_step, 0)
    for u in range(blocks):
        merge_block(seqs - 1, u, True)
        attend_block(seqs - 1, u, True)

    def drain(s, last):
        for way in range(2):
            hop_copy(way, s).wait_send()
            for u in range(dir_blocks(last)):
                dir_copy(way, s, u, last).wait_send()
            for u in range(blocks):
                for p in range(pieces(u, last)):
                    last_copy(way, s, u, p, last).wait_send()
        for u in range(blocks):
            for p in range(pieces(u, last)):
                y_copy(s, u, p, last).wait_send()

    for rel in (2, 1, 3):
        for s in range(seqs):
            for i in range(2):
                meta_copy(rel, s, i).wait_send()
    for k in range(chips):
        for e in range(local):
            sib_copy(order(k), e).wait_send()
    for s in range(seqs):
        drain(s, s == seqs - 1)


def solution(mesh):
    ep_size, pp_size = mesh.shape['ep'], mesh.shape['pp']
    chips = ep_size // CORES
    token_spec = P(('data', 'pp'), 'ep', None, None)
    weight_spec = P('pp', None, None, None)

    def body(expert_out, expert_ids, slot_ids, gate_vals, residual, norm_scale, w_query, w_key, w_value, w_out):
        local, capacity, width = expert_out.shape[1:]
        cap = capacity // ep_size
        seqs, seq_len, tops = expert_ids.shape[1:]
        half, blocks, pieces = seq_len // 2, seq_len // BLOCK, sum(PIECES)
        assert len(PIECES) == blocks and cap // 2 < -NONE
        heads, head_dim = w_query.shape[2:]
        routing = [jnp.swapaxes(a[0], 1, 2) for a in (expert_ids, slot_ids, gate_vals)]

        def flat_t(w):
            return jnp.transpose(w[0], (1, 2, 0)).reshape(heads * head_dim, width)

        dims = (chips, pp_size, seqs, seq_len, cap, local, head_dim)
        dma = pltpu.SemaphoreType.DMA
        any_spec = pl.BlockSpec(memory_space=pl.ANY)
        vmem_spec = pl.BlockSpec(memory_space=pltpu.VMEM)
        result = pl.pallas_call(
            functools.partial(stage_kernel, dims),
            out_shape=pltpu.VMEM((seqs, seq_len, width), BF16),
            in_specs=[any_spec] * 5 + [vmem_spec] + [any_spec] * 4,
            out_specs=vmem_spec,
            scratch_shapes=[
                pltpu.VMEM((seqs, tops, seq_len), jnp.int32),
                pltpu.VMEM((seqs, tops, seq_len), jnp.int32),
                pltpu.VMEM((seqs, tops, seq_len), F32),
                pltpu.VMEM((chips, seqs, CORES * local, seq_len), BF16),
                pltpu.VMEM((chips, seqs, CORES * local, seq_len), F32),
                pltpu.VMEM((chips, seqs, CORES * local, seq_len), BF16),
                pltpu.VMEM((chips, seqs, CORES * local, seq_len), F32),
                pltpu.VMEM((2, local, cap, width), BF16),
                pltpu.VMEM((chips, local, cap, width), BF16),
                pltpu.VMEM((chips, seqs, 2, half, width), F32),
                pltpu.VMEM((2, seqs, half, width), F32),
                pltpu.VMEM((2, seqs, half, width), F32),
                pltpu.VMEM((2, seqs, half, width), F32),
                pltpu.VMEM((seqs, seq_len, width), BF16),
                pltpu.VMEM((seqs, seq_len, width), BF16),
                pltpu.VMEM((seqs, seq_len, width), BF16),
                dma((3,)), dma((2, chips, seqs)), dma((2, chips, seqs)), dma((chips, local)), dma((chips, local)), dma((2,)), dma, dma((4, local)),
                dma((2, seqs)), dma((2, seqs)), dma((2, seqs, blocks)), dma((2, seqs, blocks)),
                dma((2, seqs, pieces)), dma((2, seqs, pieces)), dma((seqs, pieces)), dma((seqs, pieces)),
            ],
            compiler_params=pltpu.CompilerParams(collective_id=0, has_side_effects=True, vmem_limit_bytes=64200000),
            name='stage',
        )(*routing, expert_out[0], residual[0], norm_scale, flat_t(w_query), flat_t(w_key), flat_t(w_value),
          w_out[0].reshape(heads * head_dim, width))
        return result[None]

    return jax.shard_map(body, mesh=mesh, in_specs=(token_spec, token_spec, token_spec, token_spec, token_spec, P('pp', None), weight_spec, weight_spec, weight_spec, weight_spec), out_specs=token_spec, check_vma=False)
```
